32 devices in a mesh: seq: 8 (over z, y), head: 4 (over x, core).
Axes of the slice: x: 2, y: 2, z: 4, core: 2. Of those that a mesh axis runs over, the one named last changes fastest.
Arguments:
- tail_queries: bfloat16 [10, 64, 4096], P(None, 'seq', 'head'), may hold values from -8 to 8
- keys: bfloat16 [10, 16384, 1024], P(None, 'seq', 'head'), may hold values from -160 to 160
Outputs:
- vertical: float32 [10, 32, 16384], P(None, 'head', 'seq')
- slash: float32 [10, 32, 16384], P(None, 'head', 'seq')
The draws below stay inside these ranges and needn't reach their ends.
All inputs are finite; a program needn't handle non-finite values.
Results may differ from the reference program's by a relative error of at most 0.0003.
Values may be sent and summed in bfloat16 or wider, within the bound.
A program may use at most 64 MiB of HBM per device.

```python
import math
import jax
import jax.numpy as jnp
from jax import lax

HD = 128
HEADS = 32
KV_HEADS = 8
LAST = 64
LAYERS = 10
TOKENS = 16384


def query_field(key):
    return jax.random.normal(jax.random.fold_in(key, 11), (LAYERS, LAST, HEADS * HD), jnp.float32)


def draw_tail_queries(key, part):
    return query_field(key).astype(jnp.bfloat16)


def draw_keys(key, part):
    normal_keys = jax.random.normal(jax.random.fold_in(key, 23), (LAYERS, TOKENS, KV_HEADS * HD), jnp.float32)
    return normal_keys.astype(jnp.bfloat16)


def setup_inputs(seed: int = 0) -> dict:
    streams_of = jax.random.split(jax.random.key(seed), 3)
    return {
        "tail_queries": draw_tail_queries(jax.random.fold_in(streams_of[2], 71), 0),
        "keys": draw_keys(jax.random.fold_in(streams_of[2], 71), 0),
    }


def diagonal_sums(probabilities):
    head_count, query_count, key_count = probabilities.shape
    width = key_count + (query_count + 127) // 128 * 128
    rows = jnp.pad(probabilities[:, ::-1, :], ((0, 0), (0, 0), (0, width - key_count)))
    offset = 1
    while rows.shape[1] > 1:
        if rows.shape[1] % 2 == 1:
            rows = jnp.pad(rows, ((0, 0), (0, 1), (0, 0)))
        even_rows = rows[:, 0::2, :]
        odd_rows = rows[:, 1::2, :]
        odd_rows = jnp.pad(odd_rows[:, :, :width - offset], ((0, 0), (0, 0), (offset, 0)))
        rows = even_rows + odd_rows
        offset = offset * 2
    return rows[:, 0, :key_count + query_count]

def group_sums(inputs):
    queries, group_keys = inputs
    scores = jnp.einsum('qad,kd->aqk', queries.astype(jnp.float32), group_keys.astype(jnp.float32), precision=lax.Precision.HIGHEST)
    scores = scores * (1.0 / math.sqrt(HD))
    positions = TOKENS - LAST + jnp.arange(LAST)
    visible = jnp.arange(TOKENS)[None, :] <= positions[:, None]
    scores = jnp.where(visible[None], scores, -jnp.inf)
    row_max = lax.optimization_barrier(jnp.max(scores, axis=2, keepdims=True))
    weights = jnp.exp(scores - row_max)
    row_total = lax.optimization_barrier(jnp.sum(weights, axis=2, keepdims=True))
    probabilities = weights / row_total
    ratio = TOKENS / LAST
    vertical = lax.optimization_barrier(jnp.sum(probabilities, axis=1)) * ratio
    slash = diagonal_sums(probabilities)[:, :TOKENS] * ratio
    return (vertical, slash)

def layer_sums(inputs):
    queries, layer_keys = inputs
    per_group = HEADS // KV_HEADS
    grouped_queries = queries.reshape(LAST, KV_HEADS, per_group, HD).transpose(1, 0, 2, 3)
    grouped_keys = layer_keys.reshape(TOKENS, KV_HEADS, HD).transpose(1, 0, 2)
    vertical, slash = lax.map(group_sums, (grouped_queries, grouped_keys))
    return (vertical.reshape(HEADS, TOKENS), slash.reshape(HEADS, TOKENS))

def reference(tail_queries, keys):
    vertical, slash = lax.map(layer_sums, (tail_queries, keys))
    return (vertical, slash)
```

```python
import functools
import math

import jax
import jax.numpy as jnp
from jax import lax
from jax.experimental import pallas as pl
from jax.experimental.pallas import tpu as pltpu
from jax.sharding import PartitionSpec as P

HD = 128
LAST = 64
LANES = 128
LAG = 4
KEY_SLOTS = 3
BLOCK = 8
SCORE_COLUMNS = 512


def kernel(
    n, fast, q_ref, k_ref, vert_ref, slash_ref,
    qg, kbuf, w, st_tx, st_rx, ov_tx, ov_rx,
    own_sem, k_sem, zs, zr, ys, yr, ss, sr, osem, orsem,
):
    layers, rows, _ = q_ref.shape
    key_count = k_ref.shape[1]
    groups = k_ref.shape[2] // HD
    heads = rows * n // LAST
    per_group = heads // groups
    tiles = key_count // LANES
    slow = n // fast
    slots = LAG + 1
    tokens = key_count * n
    scale = math.log2(math.e) / math.sqrt(HD)
    ratio = tokens / LAST

    me = lax.axis_index("seq")
    my_slow = lax.div(me, fast)
    my_fast = lax.rem(me, fast)
    lane = lax.broadcasted_iota(jnp.int32, (heads, LANES), 1)

    def remote(src, dst, send, recv, dest):
        return pltpu.make_async_remote_copy(
            src_ref=src, dst_ref=dst, send_sem=send, recv_sem=recv,
            device_id={"seq": dest}, device_id_type=pl.DeviceIdType.MESH,
        )

    def wait_for(ref, sem):
        pltpu.make_async_copy(ref, ref, sem).wait()

    def key_copy(layer):
        slot = lax.rem(layer, KEY_SLOTS)
        return pltpu.make_async_copy(k_ref.at[layer], kbuf.at[slot], k_sem.at[slot])

    for layer in range(min(KEY_SLOTS - 1, layers)):
        key_copy(jnp.int32(layer)).start()
    own_copy = pltpu.make_async_copy(q_ref, qg.at[:, me], own_sem)
    own_copy.start()

    barrier = pltpu.get_barrier_semaphore()
    for d in range(1, n):
        pl.semaphore_signal(
            barrier, inc=1, device_id={"seq": lax.rem(me + d, n)},
            device_id_type=pl.DeviceIdType.MESH,
        )
    pl.semaphore_wait(barrier, n - 1)

    partner = my_slow * fast + lax.rem(my_fast + 1, fast)

    def send_queries(layer, carry):
        for d in range(1, slow):
            dest = lax.rem(my_slow + d, slow) * fast + my_fast
            remote(q_ref.at[layer], qg.at[layer, me], zs.at[layer], zr.at[layer], dest).start()
        if fast > 1:
            remote(q_ref.at[layer], qg.at[layer, me], ys.at[layer], yr.at[layer], partner).start()
        return carry

    lax.fori_loop(0, layers, send_queries, 0)

    def forward_queries(layer):
        if slow > 1:
            wait_for(qg.at[layer, pl.ds(0, slow - 1)], zr.at[layer])
            if fast > 1:
                for d in range(1, slow):
                    src = lax.rem(my_slow + d, slow) * fast + my_fast
                    block = qg.at[layer, src]
                    remote(block, block, ys.at[layer], yr.at[layer], partner).start()

    own_copy.wait()
    forward_queries(jnp.int32(0))

    def first_pass(layer):
        slot = lax.rem(layer, slots)
        queries = qg[layer].astype(jnp.float32).reshape(n * rows, HD)
        head = lax.rem(lax.broadcasted_iota(jnp.int32, (n * rows, HD), 0), heads)
        pieces = [
            jnp.where((head >= g * per_group) & (head < (g + 1) * per_group), queries, 0.0)
            for g in range(groups)
        ]
        spread_queries = jnp.concatenate(pieces, axis=1).astype(jnp.bfloat16)
        key_slot = lax.rem(layer, KEY_SLOTS)
        for c in range(0, key_count, SCORE_COLUMNS):
            w[slot, :, c : c + SCORE_COLUMNS] = lax.dot_general(
                spread_queries, kbuf[key_slot, c : c + SCORE_COLUMNS, :],
                (((1,), (1,)), ((), ())), preferred_element_type=jnp.float32,
            )
        limit = tokens - LAST - (me * key_count + key_count - LANES)

        def normalise(block, stats):
            maxima = []
            for u in range(BLOCK):
                i = block * BLOCK + u
                at = pl.ds(pl.multiple_of(i * heads, heads), heads)
                last = w[slot, at, key_count - LANES :]
                last = jnp.where(lane <= limit + i, last, -jnp.inf)
                w[slot, at, key_count - LANES :] = last
                top = last
                for t in range(tiles - 1):
                    top = jnp.maximum(top, w[slot, at, t * LANES : (t + 1) * LANES])
                maxima.append(jnp.max(top, axis=1, keepdims=True))
            for u in range(BLOCK):
                i = block * BLOCK + u
                at = pl.ds(pl.multiple_of(i * heads, heads), heads)
                top = jnp.broadcast_to(maxima[u], (heads, LANES))
                total = None
                for t in range(tiles):
                    cols = slice(t * LANES, (t + 1) * LANES)
                    weight = jnp.exp2((w[slot, at, cols] - top) * scale)
                    w[slot, at, cols] = weight
                    total = weight if total is None else total + weight
                total = jnp.sum(total, axis=1, keepdims=True)
                stats = jnp.where(lane == i, top, stats)
                stats = jnp.where(lane == LAST + i, total, stats)
            return stats

        st_tx[layer] = lax.fori_loop(
            0, LAST // BLOCK, normalise, jnp.zeros((heads, LANES), jnp.float32)
        )

    def shifted(before, now, steps):
        return jnp.where(lane < steps, before, now)

    def second_pass(layer):
        slot = lax.rem(layer, slots)
        if n > 1:
            wait_for(st_rx.at[layer, pl.ds(0, n - 1)], sr.at[layer])
        own = st_tx[layer]
        others = [st_rx[layer, lax.rem(me + d, n)] for d in range(1, n)]
        top = functools.reduce(jnp.maximum, others, own)
        mine = jnp.exp2((own - top) * scale)
        total = pltpu.roll(own, LAST, 1) * mine
        for other in others:
            total += pltpu.roll(other, LAST, 1) * jnp.exp2((other - top) * scale)
        factor = mine / total * ratio

        zero = jnp.zeros((heads, LANES), jnp.float32)
        for t in range(tiles):
            cols = slice(t * LANES, (t + 1) * LANES)
            vert_ref[layer, :, cols] = zero
            slash_ref[layer, :, cols] = zero
        ov_tx[layer] = zero

        def gather_block(block, factor):
            scales = [
                jnp.broadcast_to(factor[:, u : u + 1], (heads, LANES)) for u in range(BLOCK)
            ]
            before = {}
            for t in range(tiles + 1):
                cols = slice(t * LANES, (t + 1) * LANES)
                if t < tiles:
                    level = []
                    for u in range(BLOCK):
                        at = pl.ds(pl.multiple_of((block * BLOCK + u) * heads, heads), heads)
                        level.append(w[slot, at, cols] * scales[u])
                    vert_ref[layer, :, cols] += functools.reduce(jnp.add, level)
                else:
                    level = [None] * BLOCK
                steps = 1
                while len(level) > 1:
                    following = []
                    for a in range(0, len(level), 2):
                        now = zero if level[a] is None else pltpu.roll(level[a], steps, 1)
                        value = shifted(before.get((steps, a), zero), now, steps)
                        before[steps, a] = now
                        following.append(value if level[a + 1] is None else value + level[a + 1])
                    level = following
                    steps *= 2
                old = slash_ref[layer, :, cols] if t < tiles else ov_tx[layer]
                now = pltpu.roll(old, BLOCK, 1)
                value = shifted(before.get("acc", zero), now, BLOCK) + level[0]
                before["acc"] = now
                if t < tiles:
                    slash_ref[layer, :, cols] = value
                else:
                    ov_tx[layer] = value
            return pltpu.roll(factor, LANES - BLOCK, 1)

        lax.fori_loop(0, LAST // BLOCK, gather_block, factor)

    def send_stats(layer):
        for d in range(1, n):
            dest = lax.rem(me + d, n)
            remote(st_tx.at[layer], st_rx.at[layer, me], ss.at[layer], sr.at[layer], dest).start()

    def overflow_copy(layer):
        return remote(
            ov_tx.at[layer], ov_rx.at[layer], osem.at[layer], orsem.at[layer],
            lax.rem(me + 1, n),
        )

    def add_overflow(layer):
        @pl.when(me > 0)
        def _():
            overflow_copy(layer).wait_recv()
            slash_ref[layer, :, :LANES] += ov_rx[layer]

    def step(it, carry):
        @pl.when((it > LAG) & (it <= layers + LAG) & (me < n - 1))
        def _():
            overflow_copy(it - LAG - 1).start()

        @pl.when(it + 1 < layers)
        def _():
            forward_queries(it + 1)

        @pl.when(it < layers)
        def _():
            @pl.when(it + KEY_SLOTS - 1 < layers)
            def _():
                key_copy(it + KEY_SLOTS - 1).start()

            if fast > 1:
                wait_for(qg.at[it, pl.ds(0, slow)], yr.at[it])
            key_copy(it).wait()
            first_pass(it)

        @pl.when((it >= LAG) & (it < layers + LAG))
        def _():
            second_pass(it - LAG)

        @pl.when(it < layers)
        def _():
            send_stats(it)

        @pl.when(it >= LAG + 2)
        def _():
            add_overflow(it - LAG - 2)

        return carry

    lax.fori_loop(0, layers + LAG + 2, step, 0)

    def drain(layer, carry):
        if slow > 1:
            wait_for(qg.at[layer, pl.ds(0, slow - 1)], zs.at[layer])
        if fast > 1:
            wait_for(qg.at[layer, pl.ds(0, slow)], ys.at[layer])
        if n > 1:
            wait_for(st_rx.at[layer, pl.ds(0, n - 1)], ss.at[layer])

        @pl.when(me < n - 1)
        def _():
            overflow_copy(layer).wait_send()

        return carry

    lax.fori_loop(0, layers, drain, 0)


def on_device(n, fast, tail_queries, keys):
    layers, own_rows, width = tail_queries.shape
    heads = width // HD
    rows = own_rows * heads
    key_count = keys.shape[1]
    queries = tail_queries.reshape(layers, rows, HD)
    out = jax.ShapeDtypeStruct((layers, heads, key_count), jnp.float32)
    dma = pltpu.SemaphoreType.DMA
    return pl.pallas_call(
        functools.partial(kernel, n, fast),
        out_shape=(out, out),
        in_specs=[
            pl.BlockSpec(memory_space=pltpu.VMEM),
            pl.BlockSpec(memory_space=pl.ANY),
        ],
        out_specs=(
            pl.BlockSpec(memory_space=pltpu.VMEM),
            pl.BlockSpec(memory_space=pltpu.VMEM),
        ),
        scratch_shapes=[
            pltpu.VMEM((layers, n, rows, HD), jnp.bfloat16),
            pltpu.VMEM((KEY_SLOTS, key_count, keys.shape[2]), jnp.bfloat16),
            pltpu.VMEM((LAG + 1, LAST * heads, key_count), jnp.float32),
            pltpu.VMEM((layers, heads, LANES), jnp.float32),
            pltpu.VMEM((layers, n, heads, LANES), jnp.float32),
            pltpu.VMEM((layers, heads, LANES), jnp.float32),
            pltpu.VMEM((layers, heads, LANES), jnp.float32),
            dma, dma((KEY_SLOTS,)),
            dma((layers,)), dma((layers,)), dma((layers,)), dma((layers,)),
            dma((layers,)), dma((layers,)), dma((layers,)), dma((layers,)),
        ],
        compiler_params=pltpu.CompilerParams(
            collective_id=0, has_side_effects=True, vmem_limit_bytes=56 * 1024 * 1024
        ),
    )(queries, keys)


def solution(mesh):
    n = mesh.shape["seq"]
    fast = 2 if n % 2 == 0 else 1
    return jax.shard_map(
        functools.partial(on_device, n, fast),
        mesh=mesh,
        in_specs=(P(None, "seq", "head"), P(None, "seq", "head")),
        out_specs=(P(None, "head", "seq"), P(None, "head", "seq")),
        check_vma=False,
    )
```

```python
import functools
import math

import jax
import jax.numpy as jnp
from jax import lax
from jax.experimental import pallas as pl
from jax.experimental.pallas import tpu as pltpu
from jax.sharding import PartitionSpec as P

HD = 128
LAST = 64
LANES = 128
LAG = 4
KEY_SLOTS = 3
BLOCK = 8
BLOCKS = LAST // BLOCK
SLOTS = LAG + 1


def kernel(
    n, fast, q_ref, k_ref, vert_ref, slash_ref,
    qg, kbuf, qx, tops, totals, raw, w, st_tx, st_rx, ov_tx, ov_rx,
    own_sem, k_sem, zs, zr, ys, yr, ss, sr, osem, orsem,
):
    layers, rows, _ = q_ref.shape
    key_count = k_ref.shape[1]
    groups = k_ref.shape[2] // HD
    heads = rows * n // LAST
    per_group = heads // groups
    tiles = key_count // LANES
    slow = n // fast
    tokens = key_count * n
    scale = math.log2(math.e) / math.sqrt(HD)
    ratio = tokens / LAST

    me = lax.axis_index("seq")
    my_slow = lax.div(me, fast)
    my_fast = lax.rem(me, fast)
    lane = lax.broadcasted_iota(jnp.int32, (heads, LANES), 1)

    def remote(src, dst, send, recv, dest):
        return pltpu.make_async_remote_copy(
            src_ref=src, dst_ref=dst, send_sem=send, recv_sem=recv,
            device_id={"seq": dest}, device_id_type=pl.DeviceIdType.MESH,
        )

    def wait_for(ref, sem):
        pltpu.make_async_copy(ref, ref, sem).wait()

    def key_copy(layer):
        slot = layer % KEY_SLOTS
        return pltpu.make_async_copy(k_ref.at[layer], kbuf.at[slot], k_sem.at[slot])

    for layer in range(min(KEY_SLOTS - 1, layers)):
        key_copy(layer).start()
    own_copy = pltpu.make_async_copy(q_ref, qg.at[:, me], own_sem)
    own_copy.start()

    barrier = pltpu.get_barrier_semaphore()
    for d in range(1, n):
        pl.semaphore_signal(
            barrier, inc=1, device_id={"seq": lax.rem(me + d, n)},
            device_id_type=pl.DeviceIdType.MESH,
        )
    pl.semaphore_wait(barrier, n - 1)

    partner = my_slow * fast + lax.rem(my_fast + 1, fast)

    def send_queries(layer, carry):
        for d in range(1, slow):
            dest = lax.rem(my_slow + d, slow) * fast + my_fast
            remote(q_ref.at[layer], qg.at[layer, me], zs.at[layer], zr.at[layer], dest).start()
        if fast > 1:
            remote(q_ref.at[layer], qg.at[layer, me], ys.at[layer], yr.at[layer], partner).start()
        return carry

    lax.fori_loop(0, layers, send_queries, 0)

    def forward_queries(layer):
        if slow > 1:
            wait_for(qg.at[layer, pl.ds(0, slow - 1)], zr.at[layer])
            if fast > 1:
                for d in range(1, slow):
                    src = lax.rem(my_slow + d, slow) * fast + my_fast
                    block = qg.at[layer, src]
                    remote(block, block, ys.at[layer], yr.at[layer], partner).start()

    own_copy.wait()
    forward_queries(0)

    limit = tokens - LAST - (me * key_count + key_count - LANES)
    last_tile = tiles - 1

    def spread_queries(layer):
        queries = qg[layer].astype(jnp.float32).reshape(n * rows, HD)
        head = lax.rem(lax.broadcasted_iota(jnp.int32, (n * rows, HD), 0), heads)
        pieces = [
            jnp.where((head >= g * per_group) & (head < (g + 1) * per_group), queries, 0.0)
            for g in range(groups)
        ]
        qx[...] = jnp.concatenate(pieces, axis=1).astype(jnp.bfloat16)

    def block_rows(block, u):
        return pl.ds(pl.multiple_of((block * BLOCK + u) * heads, heads), heads)

    def score_block(layer, block):
        width = key_count // BLOCKS
        at = pl.ds(pl.multiple_of(block * width, width), width)
        raw[layer % 2][:, at] = lax.dot_general(
            qx[...], kbuf[layer % KEY_SLOTS, at, :],
            (((1,), (1,)), ((), ())), preferred_element_type=jnp.float32,
        )

    def load_score(layer, block, u, t):
        value = raw[layer % 2][block_rows(block, u), t * LANES : (t + 1) * LANES]
        if t == last_tile:
            value = jnp.where(lane <= limit + block * BLOCK + u, value, -jnp.inf)
        return value

    def row_top(layer, block, u, stats):
        top = load_score(layer, block, u, 0)
        for t in range(1, tiles):
            top = jnp.maximum(top, load_score(layer, block, u, t))
        top = jnp.broadcast_to(jnp.max(top, axis=1, keepdims=True), (heads, LANES))
        tops[u] = top
        return jnp.where(lane == block * BLOCK + u, top, stats)

    def row_weights(layer, block, u, top):
        at = block_rows(block, u)
        sums = [None] * 2
        for t in range(tiles):
            weight = jnp.exp2((load_score(layer, block, u, t) - top) * scale)
            w[layer % SLOTS][at, t * LANES : (t + 1) * LANES] = weight
            sums[t % 2] = weight if sums[t % 2] is None else sums[t % 2] + weight
        totals[u] = sums[0] + sums[1]

    def row_total(block, u, total, stats):
        total = jnp.sum(total, axis=1, keepdims=True)
        return jnp.where(lane == LAST + block * BLOCK + u, total, stats)

    def shifted(before, now, steps):
        return jnp.where(lane < steps, before, now)

    def factors(layer):
        if n > 1:
            wait_for(st_rx.at[layer, pl.ds(0, n - 1)], sr.at[layer])
        own = st_tx[layer]
        others = [st_rx[layer, lax.rem(me + d, n)] for d in range(1, n)]
        top = functools.reduce(jnp.maximum, others, own)
        mine = jnp.exp2((own - top) * scale)
        total = pltpu.roll(own, LAST, 1) * mine
        for other in others:
            total += pltpu.roll(other, LAST, 1) * jnp.exp2((other - top) * scale)
        return mine / total * ratio

    zero = jnp.zeros((heads, LANES), jnp.float32)

    def clear_sums(layer):
        for t in range(tiles):
            cols = slice(t * LANES, (t + 1) * LANES)
            vert_ref[layer, :, cols] = zero
            slash_ref[layer, :, cols] = zero
        ov_tx[layer] = zero

    def tree_sum(values):
        while len(values) > 1:
            pairs = [a + b for a, b in zip(values[::2], values[1::2])]
            values = pairs + values[len(pairs) * 2 :]
        return values[0]

    def sum_tile(layer, block, t, scales, before):
        cols = slice(t * LANES, (t + 1) * LANES)
        if t < tiles:
            level = [
                w[layer % SLOTS][block_rows(block, u), cols] * scales[u] for u in range(BLOCK)
            ]
            vert_ref[layer, :, cols] += tree_sum(level)
        moved = []
        for u in range(BLOCK - 1):
            steps = BLOCK - 1 - u
            now = zero if t == tiles else pltpu.roll(level[u], steps, 1)
            moved.append(shifted(before.get(u, zero), now, steps))
            before[u] = now
        if t < tiles:
            moved.append(level[-1])
        moved = tree_sum(moved)
        old = slash_ref[layer, :, cols] if t < tiles else ov_tx[layer]
        now = pltpu.roll(old, BLOCK, 1)
        value = shifted(before.get("acc", zero), now, BLOCK) + moved
        before["acc"] = now
        if t < tiles:
            slash_ref[layer, :, cols] = value
        else:
            ov_tx[layer] = value

    def compute(score, weigh, gather):
        factor = first_stats = zero
        if score is not None:
            spread_queries(score)
        if weigh is not None:
            for u in range(BLOCK):
                first_stats = row_top(weigh, 0, u, first_stats)
                totals[u] = zero
        if gather is not None:
            factor = factors(gather)
            clear_sums(gather)

        def body(block, carry):
            stats, factor = carry
            scales = [
                jnp.broadcast_to(factor[:, u : u + 1], (heads, LANES)) for u in range(BLOCK)
            ] if gather is not None else None
            before = {}
            if weigh is not None:
                old_tops = [tops[u] for u in range(BLOCK)]
                old_totals = [totals[u] for u in range(BLOCK)]
                following = lax.rem(block + 1, BLOCKS)
                for u in range(BLOCK):
                    kept = row_total(block - 1, u, old_totals[u], stats)
                    stats = jnp.where(block > 0, kept, stats)
            if score is not None:
                score_block(score, block)
            done = 0
            for u in range(BLOCK):
                if weigh is not None:
                    stats = row_top(weigh, following, u, stats)
                    row_weights(weigh, block, u, old_tops[u])
                if gather is not None:
                    until = (tiles + 1) * (u + 1) // BLOCK
                    for t in range(done, until):
                        sum_tile(gather, block, t, scales, before)
                    done = until
            if gather is not None:
                factor = pltpu.roll(factor, LANES - BLOCK, 1)
            return stats, factor

        stats, _ = lax.fori_loop(0, BLOCKS, body, (first_stats, factor))
        if weigh is not None:
            for u in range(BLOCK):
                stats = row_total(BLOCKS - 1, u, totals[u], stats)
            st_tx[weigh] = stats

    def send_stats(layer):
        for d in range(1, n):
            dest = lax.rem(me + d, n)
            remote(st_tx.at[layer], st_rx.at[layer, me], ss.at[layer], sr.at[layer], dest).start()

    def overflow_copy(layer):
        return remote(
            ov_tx.at[layer], ov_rx.at[layer], osem.at[layer], orsem.at[layer],
            lax.rem(me + 1, n),
        )

    def add_overflow(layer):
        @pl.when(me > 0)
        def _():
            overflow_copy(layer).wait_recv()
            slash_ref[layer, :, :LANES] += ov_rx[layer]

    def send_overflow(layer):
        @pl.when(me < n - 1)
        def _():
            overflow_copy(layer).start()

    def within(layer):
        return layer if 0 <= layer < layers else None

    for it in range(layers + LAG):
        score, weigh, gather = within(it), within(it - 1), within(it - LAG)
        if within(it + 1) is not None:
            forward_queries(it + 1)
        if score is not None:
            if it + KEY_SLOTS - 1 < layers:
                key_copy(it + KEY_SLOTS - 1).start()
            if fast > 1:
                wait_for(qg.at[it, pl.ds(0, slow)], yr.at[it])
            key_copy(it).wait()
        compute(score, weigh, gather)
        if gather is not None:
            send_overflow(gather)
        if weigh is not None:
            send_stats(weigh)
        if within(gather - 2 if gather is not None else -1) is not None:
            add_overflow(gather - 2)
    for layer in range(max(layers - 2, 0), layers):
        add_overflow(layer)

    def drain(layer, carry):
        if slow > 1:
            wait_for(qg.at[layer, pl.ds(0, slow - 1)], zs.at[layer])
        if fast > 1:
            wait_for(qg.at[layer, pl.ds(0, slow)], ys.at[layer])
        if n > 1:
            wait_for(st_rx.at[layer, pl.ds(0, n - 1)], ss.at[layer])

        @pl.when(me < n - 1)
        def _():
            overflow_copy(layer).wait_send()

        return carry

    lax.fori_loop(0, layers, drain, 0)


def on_device(n, fast, tail_queries, keys):
    layers, own_rows, width = tail_queries.shape
    heads = width // HD
    rows = own_rows * heads
    key_count = keys.shape[1]
    queries = tail_queries.reshape(layers, rows, HD)
    out = jax.ShapeDtypeStruct((layers, heads, key_count), jnp.float32)
    dma = pltpu.SemaphoreType.DMA
    return pl.pallas_call(
        functools.partial(kernel, n, fast),
        out_shape=(out, out),
        in_specs=[
            pl.BlockSpec(memory_space=pltpu.VMEM),
            pl.BlockSpec(memory_space=pl.ANY),
        ],
        out_specs=(
            pl.BlockSpec(memory_space=pltpu.VMEM),
            pl.BlockSpec(memory_space=pltpu.VMEM),
        ),
        scratch_shapes=[
            pltpu.VMEM((layers, n, rows, HD), jnp.bfloat16),
            pltpu.VMEM((KEY_SLOTS, key_count, keys.shape[2]), jnp.bfloat16),
            pltpu.VMEM((LAST * heads, keys.shape[2]), jnp.bfloat16),
            pltpu.VMEM((BLOCK, heads, LANES), jnp.float32),
            pltpu.VMEM((BLOCK, heads, LANES), jnp.float32),
            [pltpu.VMEM((LAST * heads, key_count), jnp.float32)] * 2,
            [pltpu.VMEM((LAST * heads, key_count), jnp.float32)] * SLOTS,
            pltpu.VMEM((layers, heads, LANES), jnp.float32),
            pltpu.VMEM((layers, n, heads, LANES), jnp.float32),
            pltpu.VMEM((layers, heads, LANES), jnp.float32),
            pltpu.VMEM((layers, heads, LANES), jnp.float32),
            dma, dma((KEY_SLOTS,)),
            dma((layers,)), dma((layers,)), dma((layers,)), dma((layers,)),
            dma((layers,)), dma((layers,)), dma((layers,)), dma((layers,)),
        ],
        compiler_params=pltpu.CompilerParams(
            collective_id=0, has_side_effects=True, vmem_limit_bytes=56 * 1024 * 1024
        ),
    )(queries, keys)


def solution(mesh):
    n = mesh.shape["seq"]
    fast = 2 if n % 2 == 0 else 1
    return jax.shard_map(
        functools.partial(on_device, n, fast),
        mesh=mesh,
        in_specs=(P(None, "seq", "head"), P(None, "seq", "head")),
        out_specs=(P(None, "head", "seq"), P(None, "head", "seq")),
        check_vma=False,
    )
```

```python
import functools
import math

import jax
import jax.numpy as jnp
from jax import lax
from jax.experimental import pallas as pl
from jax.experimental.pallas import tpu as pltpu
from jax.sharding import PartitionSpec as P

HD = 128
LAST = 64
LANES = 128
LAG = 5
KEY_SLOTS = 3
BLOCK = 8
BLOCKS = LAST // BLOCK
SLOTS = LAG + 1


def kernel(
    n, fast, packed_ref, k_ref, vert_ref, slash_ref,
    stage, q_ref, qg, kbuf, qx, tops, totals, raw, w, st_tx, st_rx, ov_tx, ov_rx,
    k_sem, zs, zr, ys, yr, ss, sr, osem, orsem,
):
    layers, rows, _ = q_ref.shape
    key_count = k_ref.shape[1]
    groups = k_ref.shape[2] // HD
    heads = rows * n // LAST
    per_group = heads // groups
    tiles = key_count // LANES
    slow = n // fast
    tokens = key_count * n
    scale = math.log2(math.e) / math.sqrt(HD)
    ratio = tokens / LAST

    me = lax.axis_index("seq")
    my_slow = lax.div(me, fast)
    my_fast = lax.rem(me, fast)
    lane = lax.broadcasted_iota(jnp.int32, (heads, LANES), 1)

    def remote(src, dst, send, recv, dest):
        return pltpu.make_async_remote_copy(
            src_ref=src, dst_ref=dst, send_sem=send, recv_sem=recv,
            device_id={"seq": dest}, device_id_type=pl.DeviceIdType.MESH,
        )

    def wait_for(ref, sem):
        pltpu.make_async_copy(ref, ref, sem).wait()

    def key_copy(layer):
        slot = layer % KEY_SLOTS
        return pltpu.make_async_copy(k_ref.at[layer], kbuf.at[slot], k_sem.at[slot])

    for layer in range(min(KEY_SLOTS - 1, layers)):
        key_copy(layer).start()
    own_rows = packed_ref.shape[1]
    for layer in range(layers):
        for h in range(heads):
            at = pl.ds(h, own_rows, stride=heads) if own_rows > 1 else pl.ds(h, 1)
            piece = packed_ref[layer, :, h * HD : (h + 1) * HD]
            stage[layer, at, :] = piece.astype(jnp.float32)
    for layer in range(layers):
        own = stage[layer].astype(jnp.bfloat16)
        q_ref[layer] = own
        qg[layer, me] = own

    barrier = pltpu.get_barrier_semaphore()
    for d in range(1, n):
        pl.semaphore_signal(
            barrier, inc=1, device_id={"seq": lax.rem(me + d, n)},
            device_id_type=pl.DeviceIdType.MESH,
        )
    pl.semaphore_wait(barrier, n - 1)

    partner = my_slow * fast + lax.rem(my_fast + 1, fast)

    def send_queries(layer, carry):
        for d in range(1, slow):
            dest = lax.rem(my_slow + d, slow) * fast + my_fast
            remote(q_ref.at[layer], qg.at[layer, me], zs.at[layer], zr.at[layer], dest).start()
        return carry

    lax.fori_loop(0, layers, send_queries, 0)

    def forward_queries(layer):
        if fast > 1:
            remote(q_ref.at[layer], qg.at[layer, me], ys.at[layer], yr.at[layer], partner).start()
        if slow > 1:
            wait_for(qg.at[layer, pl.ds(0, slow - 1)], zr.at[layer])
            if fast > 1:
                for d in range(1, slow):
                    src = lax.rem(my_slow + d, slow) * fast + my_fast
                    block = qg.at[layer, src]
                    remote(block, block, ys.at[layer], yr.at[layer], partner).start()

    forward_queries(0)

    limit = tokens - LAST - (me * key_count + key_count - LANES)
    last_tile = tiles - 1

    def spread_queries(layer):
        queries = qg[layer].astype(jnp.float32).reshape(n * rows, HD)
        head = lax.rem(lax.broadcasted_iota(jnp.int32, (n * rows, HD), 0), heads)
        pieces = [
            jnp.where((head >= g * per_group) & (head < (g + 1) * per_group), queries, 0.0)
            for g in range(groups)
        ]
        qx[...] = jnp.concatenate(pieces, axis=1).astype(jnp.bfloat16)

    def block_rows(block, u):
        return pl.ds(pl.multiple_of((block * BLOCK + u) * heads, heads), heads)

    def score_block(layer, block):
        width = key_count // BLOCKS
        at = pl.ds(pl.multiple_of(block * width, width), width)
        raw[layer % 2][:, at] = lax.dot_general(
            qx[...], kbuf[layer % KEY_SLOTS, at, :],
            (((1,), (1,)), ((), ())), preferred_element_type=jnp.float32,
        )

    def load_score(layer, block, u, t):
        value = raw[layer % 2][block_rows(block, u), t * LANES : (t + 1) * LANES]
        if t == last_tile:
            value = jnp.where(lane <= limit + block * BLOCK + u, value, -jnp.inf)
        return value

    def row_top(layer, block, u, stats):
        top = load_score(layer, block, u, 0)
        for t in range(1, tiles):
            top = jnp.maximum(top, load_score(layer, block, u, t))
        top = jnp.broadcast_to(jnp.max(top, axis=1, keepdims=True), (heads, LANES))
        tops[u] = top
        return jnp.where(lane == block * BLOCK + u, top, stats)

    def row_weights(layer, block, u, top):
        at = block_rows(block, u)
        sums = [None] * 2
        for t in range(tiles):
            weight = jnp.exp2((load_score(layer, block, u, t) - top) * scale)
            w[layer % SLOTS][at, t * LANES : (t + 1) * LANES] = weight
            sums[t % 2] = weight if sums[t % 2] is None else sums[t % 2] + weight
        totals[u] = sums[0] + sums[1]

    def row_total(block, u, total, stats):
        total = jnp.sum(total, axis=1, keepdims=True)
        return jnp.where(lane == LAST + block * BLOCK + u, total, stats)

    def shifted(before, now, steps):
        return jnp.where(lane < steps, before, now)

    def factors(layer):
        if n > 1:
            wait_for(st_rx.at[layer, pl.ds(0, n - 1)], sr.at[layer])
        own = st_tx[layer]
        others = [st_rx[layer, lax.rem(me + d, n)] for d in range(1, n)]
        top = functools.reduce(jnp.maximum, others, own)
        mine = jnp.exp2((own - top) * scale)
        total = pltpu.roll(own, LAST, 1) * mine
        for other in others:
            total += pltpu.roll(other, LAST, 1) * jnp.exp2((other - top) * scale)
        return mine / total * ratio

    zero = jnp.zeros((heads, LANES), jnp.float32)

    def clear_sums(layer):
        for t in range(tiles):
            cols = slice(t * LANES, (t + 1) * LANES)
            vert_ref[layer, :, cols] = zero
            slash_ref[layer, :, cols] = zero
        ov_tx[layer] = zero

    def tree_sum(values):
        while len(values) > 1:
            pairs = [a + b for a, b in zip(values[::2], values[1::2])]
            values = pairs + values[len(pairs) * 2 :]
        return values[0]

    def sum_tile(layer, block, t, scales, before):
        cols = slice(t * LANES, (t + 1) * LANES)
        if t < tiles:
            level = [w[layer % SLOTS][block_rows(block, u), cols] for u in range(BLOCK)]
            vert_ref[layer, :, cols] += tree_sum([level[u] * scales[u] for u in range(BLOCK)])
        moved = []
        for u in range(BLOCK - 1):
            steps = BLOCK - 1 - u
            now = zero if t == tiles else pltpu.roll(level[u], steps, 1)
            moved.append(shifted(before.get(u, zero), now, steps) * scales[u])
            before[u] = now
        if t < tiles:
            moved.append(level[-1] * scales[-1])
        moved = tree_sum(moved)
        old = slash_ref[layer, :, cols] if t < tiles else ov_tx[layer]
        now = pltpu.roll(old, BLOCK, 1)
        value = shifted(before.get("acc", zero), now, BLOCK) + moved
        before["acc"] = now
        if t < tiles:
            slash_ref[layer, :, cols] = value
        else:
            ov_tx[layer] = value

    def compute(score, weigh, gather):
        factor = first_stats = zero
        if score is not None:
            spread_queries(score)
        if weigh is not None:
            for u in range(BLOCK):
                first_stats = row_top(weigh, 0, u, first_stats)
                totals[u] = zero
        if gather is not None:
            factor = factors(gather)
            clear_sums(gather)

        def body(block, carry):
            stats, factor = carry
            scales = [
                jnp.broadcast_to(factor[:, u : u + 1], (heads, LANES)) for u in range(BLOCK)
            ] if gather is not None else None
            before = {}
            if weigh is not None:
                old_tops = [tops[u] for u in range(BLOCK)]
                old_totals = [totals[u] for u in range(BLOCK)]
                following = lax.rem(block + 1, BLOCKS)
                for u in range(BLOCK):
                    kept = row_total(block - 1, u, old_totals[u], stats)
                    stats = jnp.where(block > 0, kept, stats)
            if score is not None:
                score_block(score, block)
            done = 0
            for u in range(BLOCK):
                if weigh is not None:
                    stats = row_top(weigh, following, u, stats)
                    row_weights(weigh, block, u, old_tops[u])
                if gather is not None:
                    until = (tiles + 1) * (u + 1) // BLOCK
                    for t in range(done, until):
                        sum_tile(gather, block, t, scales, before)
                    done = until
            if gather is not None:
                factor = pltpu.roll(factor, LANES - BLOCK, 1)
            return stats, factor

        stats, _ = lax.fori_loop(0, BLOCKS, body, (first_stats, factor))
        if weigh is not None:
            for u in range(BLOCK):
                stats = row_total(BLOCKS - 1, u, totals[u], stats)
            st_tx[weigh] = stats

    def send_stats(layer):
        for d in range(1, n):
            dest = lax.rem(me + d, n)
            remote(st_tx.at[layer], st_rx.at[layer, me], ss.at[layer], sr.at[layer], dest).start()

    def overflow_copy(layer):
        return remote(
            ov_tx.at[layer], ov_rx.at[layer], osem.at[layer], orsem.at[layer],
            lax.rem(me + 1, n),
        )

    def add_overflow(layer):
        @pl.when(me > 0)
        def _():
            overflow_copy(layer).wait_recv()
            slash_ref[layer, :, :LANES] += ov_rx[layer]

    def send_overflow(layer):
        @pl.when(me < n - 1)
        def _():
            overflow_copy(layer).start()

    def within(layer):
        return layer if 0 <= layer < layers else None

    for it in range(layers + LAG):
        score, weigh, gather = within(it), within(it - 1), within(it - LAG)
        if within(it + 1) is not None:
            forward_queries(it + 1)
        if score is not None:
            if it + KEY_SLOTS - 1 < layers:
                key_copy(it + KEY_SLOTS - 1).start()
            if fast > 1:
                wait_for(qg.at[it, pl.ds(0, slow)], yr.at[it])
            key_copy(it).wait()
        compute(score, weigh, gather)
        if gather is not None:
            send_overflow(gather)
        if weigh is not None:
            send_stats(weigh)
        if within(gather - 2 if gather is not None else -1) is not None:
            add_overflow(gather - 2)
    for layer in range(max(layers - 2, 0), layers):
        add_overflow(layer)

    def drain(layer, carry):
        if slow > 1:
            wait_for(qg.at[layer, pl.ds(0, slow - 1)], zs.at[layer])
        if fast > 1:
            wait_for(qg.at[layer, pl.ds(0, slow)], ys.at[layer])
        if n > 1:
            wait_for(st_rx.at[layer, pl.ds(0, n - 1)], ss.at[layer])

        @pl.when(me < n - 1)
        def _():
            overflow_copy(layer).wait_send()

        return carry

    lax.fori_loop(0, layers, drain, 0)


def put_out(vertical_ref, slash_ref, vertical_out, slash_out, sems):
    copies = [
        pltpu.make_async_copy(vertical_ref, vertical_out, sems.at[0]),
        pltpu.make_async_copy(slash_ref, slash_out, sems.at[1]),
    ]
    for copy in copies:
        copy.start()
    for copy in copies:
        copy.wait()


def on_device(n, fast, tail_queries, keys):
    layers, own_rows, width = tail_queries.shape
    heads = width // HD
    rows = own_rows * heads
    key_count = keys.shape[1]
    out = jax.ShapeDtypeStruct((layers, heads, key_count), jnp.float32)
    dma = pltpu.SemaphoreType.DMA
    vertical, slash = pl.pallas_call(
        functools.partial(kernel, n, fast),
        out_shape=(out, out),
        in_specs=[
            pl.BlockSpec(memory_space=pltpu.VMEM),
            pl.BlockSpec(memory_space=pl.ANY),
        ],
        out_specs=(
            pl.BlockSpec(memory_space=pltpu.VMEM),
            pl.BlockSpec(memory_space=pltpu.VMEM),
        ),
        scratch_shapes=[
            pltpu.VMEM((layers, rows, HD), jnp.float32),
            pltpu.VMEM((layers, rows, HD), jnp.bfloat16),
            pltpu.VMEM((layers, n, rows, HD), jnp.bfloat16),
            pltpu.VMEM((KEY_SLOTS, key_count, keys.shape[2]), jnp.bfloat16),
            pltpu.VMEM((LAST * heads, keys.shape[2]), jnp.bfloat16),
            pltpu.VMEM((BLOCK, heads, LANES), jnp.float32),
            pltpu.VMEM((BLOCK, heads, LANES), jnp.float32),
            [pltpu.VMEM((LAST * heads, key_count), jnp.float32)] * 2,
            [pltpu.VMEM((LAST * heads, key_count), jnp.float32)] * SLOTS,
            pltpu.VMEM((layers, heads, LANES), jnp.float32),
            pltpu.VMEM((layers, n, heads, LANES), jnp.float32),
            pltpu.VMEM((layers, heads, LANES), jnp.float32),
            pltpu.VMEM((layers, heads, LANES), jnp.float32),
            dma((KEY_SLOTS,)),
            dma((layers,)), dma((layers,)), dma((layers,)), dma((layers,)),
            dma((layers,)), dma((layers,)), dma((layers,)), dma((layers,)),
        ],
        compiler_params=pltpu.CompilerParams(
            collective_id=0, has_side_effects=True,
            vmem_limit_bytes=56 * 1024 * 1024
        ),
    )(tail_queries, keys)
    return pl.pallas_call(
        put_out,
        out_shape=(out, out),
        in_specs=[pl.BlockSpec(memory_space=pltpu.VMEM)] * 2,
        out_specs=(pl.BlockSpec(memory_space=pl.ANY), pl.BlockSpec(memory_space=pl.ANY)),
        scratch_shapes=[dma((2,))],
        compiler_params=pltpu.CompilerParams(vmem_limit_bytes=4 * 1024 * 1024),
    )(vertical, slash)


def solution(mesh):
    n = mesh.shape["seq"]
    fast = 2 if n % 2 == 0 else 1
    return jax.shard_map(
        functools.partial(on_device, n, fast),
        mesh=mesh,
        in_specs=(P(None, "seq", "head"), P(None, "seq", "head")),
        out_specs=(P(None, "head", "seq"), P(None, "head", "seq")),
        check_vma=False,
    )
```
